32 devices in a mesh: band: 16 (over z, y, core), grid: 2 (over x).
Axes of the slice: x: 2, y: 2, z: 4, core: 2. Of those that a mesh axis runs over, the one named last changes fastest.
Arguments:
- orbitals: float32 [32, 64, 4096], P('band', 'grid'), may hold values from -4 to 4
- pair_list: int32 [16, 4, 2], P('band'), may hold values from 0 to 31, as said below
- pair_count: int32 [16], P('band'), may hold values from 1 to 4, 32 in all
Outputs:
- exchange_proj: float32 [32, 64, 4096], P('band', 'grid')
The draws below stay inside these ranges and needn't reach their ends.
Inputs may be any that keep to these rules, and one draw needn't show every extreme that they name: `pair_list`: entry 0 is an orbital index 0 to 1 within the row's band group; entry 1 is a global orbital index owned by the same band group or by one of the next 2 groups, counted cyclically; the two never name the same orbital. Band group b uses its first pair_count[b] slots.
All inputs are finite; a program needn't handle non-finite values.
Results may differ from the reference program's by a relative error of at most 0.0003.
Values sent between devices are 32-bit elements; how exact they have to be, the bound alone decides.
A program may use at most 64 MiB of HBM per device.

```python
import math
import jax
import jax.numpy as jnp
import numpy as np
from jax import lax

CELL_SPAN_COUNT = 64
ORB_DEV = 2
PAIR_MEAN = 2
REACH = 2
SLOTS = 4
NORB = 32
N_BAND = 16


def draw_orbitals(key, part):
    lattice_position = jnp.arange(CELL_SPAN_COUNT).astype(jnp.float32)
    spread = CELL_SPAN_COUNT / 4.0

    def single(number):
        folded = jax.random.fold_in(jax.random.fold_in(key, 7001), number)
        key_centre, key_wave, key_phase, key_rough = jax.random.split(folded, 4)
        centre = jax.random.uniform(key_centre, (3,), minval=0.0, maxval=float(CELL_SPAN_COUNT))
        offsets = jnp.abs(lattice_position[None, :] - centre[:, None])
        offsets = jnp.minimum(offsets, CELL_SPAN_COUNT - offsets)
        radius = offsets[0][:, None, None] ** 2 + offsets[1][None, :, None] ** 2 + offsets[2][None, None, :] ** 2
        bell_shaped_decay = jnp.exp(-radius / (2.0 * spread * spread))
        fourier_modes = jax.random.randint(key_wave, (3,), 2, CELL_SPAN_COUNT * 5 // 16 + 1).astype(jnp.float32)
        angular_displacements = jax.random.uniform(key_phase, (3,), minval=0.0, maxval=2.0 * math.pi)
        oscillating_sinusoids = jnp.cos(fourier_modes[:, None] * lattice_position[None, :] * (2.0 * math.pi / CELL_SPAN_COUNT) + angular_displacements[:, None])
        oscillating_sinusoid = oscillating_sinusoids[0][:, None, None] * oscillating_sinusoids[1][None, :, None] * oscillating_sinusoids[2][None, None, :]
        random_perturbation = jnp.clip(0.5 * jax.random.normal(key_rough, (CELL_SPAN_COUNT, CELL_SPAN_COUNT, CELL_SPAN_COUNT)), -0.9, 0.9)
        electron_function_samples = jnp.clip(2.5 * bell_shaped_decay * (oscillating_sinusoid + 0.45 * random_perturbation), -4.0, 4.0)
        return electron_function_samples.reshape(CELL_SPAN_COUNT, CELL_SPAN_COUNT * CELL_SPAN_COUNT).astype(jnp.float32)
    return lax.map(single, jnp.arange(NORB))


def draw_pair_list(key, part):
    groups = NORB // ORB_DEV
    key_first, key_hop, key_partner = jax.random.split(jax.random.fold_in(key, 7002), 3)
    first_index = jax.random.randint(key_first, (groups, SLOTS), 0, ORB_DEV)
    hop_count = jax.random.randint(key_hop, (groups, SLOTS), 0, REACH + 1)
    partner = jax.random.randint(key_partner, (groups, SLOTS), 0, ORB_DEV)
    partner = jnp.where((hop_count == 0) & (partner == first_index), (first_index + 1) % ORB_DEV, partner)
    group_ids = jnp.arange(groups, dtype=jnp.int32)[:, None]
    global_partner = (group_ids + hop_count) % groups * ORB_DEV + partner
    return jnp.stack([first_index, global_partner], axis=-1).astype(jnp.int32)


def split_up(amount, total, bound, slope):
    portions = [(1 << 20) // math.isqrt(standing ** slope) + 1 for standing in range(2, amount + 1)]
    surplus, given = total - bound - (amount - 1), [1] * (amount - 1)
    while surplus > 0:
        movable = [i for i in range(amount - 1) if given[i] < bound]
        mass, budget = sum([portions[i] for i in movable]), surplus
        for i in movable:
            addition = min(bound - given[i], max(1, budget * portions[i] // mass), surplus)
            given[i] = given[i] + addition
            surplus = surplus - addition
    return np.array([bound] + given)


def ragged_sizes(own_key, count, total, reach, skew):
    if count == 2:
        one = jax.random.randint(own_key, (), max(1, total - reach), min(reach, total - 1) + 1)
        return jnp.stack([one, total - one])
    sizes = jnp.asarray(split_up(count, total, reach, skew), jnp.int32)
    pairs = (count - 1) // 2
    source_of, receiver = sizes[1:1 + 2 * pairs:2], sizes[2:2 + 2 * pairs:2]
    margin = jnp.minimum(source_of - 1, reach - receiver)
    shifted = jax.random.randint(jax.random.fold_in(own_key, 1), (pairs,), 0, 1 << 20) % (margin + 1)
    sizes = sizes.at[1:1 + 2 * pairs:2].set(source_of - shifted).at[2:2 + 2 * pairs:2].set(receiver + shifted)
    return sizes[jax.random.permutation(jax.random.fold_in(own_key, 2), count)]


def setup_inputs(seed: int = 0) -> dict:
    key_of = jax.random.split(jax.random.key(seed), 4)
    return {
        "orbitals": draw_orbitals(jax.random.fold_in(key_of[3], 71), 0),
        "pair_list": draw_pair_list(jax.random.fold_in(key_of[3], 71), 0),
        "pair_count": ragged_sizes(key_of[2], N_BAND, PAIR_MEAN * N_BAND, SLOTS, 2).astype(jnp.int32),
    }


def kernel_table():
    points = jnp.arange(CELL_SPAN_COUNT).astype(jnp.float32)
    eigenvalues = 2.0 - 2.0 * jnp.cos(points * (2.0 * math.pi / CELL_SPAN_COUNT))
    summed = eigenvalues[:, None, None] + eigenvalues[None, :, None] + eigenvalues[None, None, :]
    return (1.0 / CELL_SPAN_COUNT) / (1.0 / CELL_SPAN_COUNT ** 2 + summed)


def reference(orbitals, pair_list, pair_count):
    groups = pair_list.shape[0]
    slot_count = pair_list.shape[1]
    kernel = kernel_table()
    group_ids = jnp.repeat(jnp.arange(groups, dtype=jnp.int32), slot_count)
    flat = pair_list.reshape(-1, 2).astype(jnp.int32)
    first_index = (group_ids * ORB_DEV + flat[:, 0]).astype(jnp.int32)
    second = flat[:, 1].astype(jnp.int32)
    alive = (jnp.arange(slot_count)[None, :] < pair_count[:, None]).reshape(-1).astype(orbitals.dtype)

    def visit(totals, inputs):
        left_id, right_id, weight = inputs
        left_rows = orbitals[left_id]
        right_rows = orbitals[right_id]
        density = (left_rows * right_rows * weight).reshape(CELL_SPAN_COUNT, CELL_SPAN_COUNT, CELL_SPAN_COUNT)
        spectrum = jnp.fft.fftn(density) * kernel
        potential = jnp.real(jnp.fft.ifftn(spectrum)).astype(density.dtype).reshape(CELL_SPAN_COUNT, CELL_SPAN_COUNT * CELL_SPAN_COUNT)
        totals = totals.at[left_id].add(potential * right_rows)
        totals = totals.at[right_id].add(potential * left_rows)
        return totals, None

    totals, unused = lax.scan(visit, jnp.zeros(orbitals.shape, orbitals.dtype), (first_index, second, alive))
    return totals
```

```python
import math

import jax
import jax.numpy as jnp
import numpy as np
from jax import lax
from jax.experimental import pallas as pl
from jax.experimental.pallas import tpu as pltpu
from jax.sharding import PartitionSpec as P

REACH = 2
GROUP = 4


def rotated(value, axis, steps):
    count = lax.axis_size(axis)
    pairs = [(source, (source + steps) % count) for source in range(count)]
    return lax.ppermute(value, axis, pairs)


def swapped(value, axis):
    count = lax.axis_size(axis)
    return lax.ppermute(value, axis, [(source, source ^ 1) for source in range(count)])


def split(value):
    high = value.astype(jnp.bfloat16)
    return high, (value - high.astype(jnp.float32)).astype(jnp.bfloat16)


def tables(side, half_rows):
    points = np.arange(side)
    angles = (points[:, None] * points[None, :] % side) * (2.0 * math.pi / side)
    hartley = (np.cos(angles) + np.sin(angles)).astype(np.float32)
    high = hartley.astype(jnp.bfloat16)
    low = (hartley - high.astype(np.float32)).astype(jnp.bfloat16)
    eye = np.eye(2, dtype=np.float32)
    wide_high = np.kron(eye, high.astype(np.float32))
    wide_low = np.kron(eye, low.astype(np.float32))
    right = np.block([[wide_high, wide_low], [wide_high, wide_low]]).astype(jnp.bfloat16)
    left = np.concatenate([high, high, low], 1)
    eigenvalues = 2.0 - 2.0 * np.cos(points * (2.0 * math.pi / side))
    shift = 1.0 / side**2 + eigenvalues[:, None] + np.tile(eigenvalues, 2)[None, :]
    ratio = 1.0 + shift / 2 - np.sqrt(shift + shift**2 / 4)
    power = ratio**half_rows
    scale = 1.0 / side / (1.0 / ratio - ratio) / side**2
    wrap = 1.0 / (1.0 - power**4)
    decay = np.stack([ratio, power, scale, wrap]).astype(np.float32)
    return right, left, decay


def along_last(value, right):
    width = value.shape[1]
    product = jnp.dot(
        jnp.concatenate(split(value), 1), right, preferred_element_type=jnp.float32
    )
    return product[:, :width] + product[:, width:]


def along_second(planes, left):
    width = planes[0].shape[1]
    out = []
    for start in range(0, len(planes), 2):
        both = jnp.concatenate(planes[start : start + 2], 1)
        high, low = split(both)
        stacked = jnp.concatenate([high, low, high], 0)
        product = jnp.dot(left, stacked, preferred_element_type=jnp.float32)
        out.append(product[:, :width])
        out.append(product[:, width:])
    return out


def forward_kernel(chosen, window, right_ref, left_ref, decay, spectrum, moments):
    slots, rows, side, width = spectrum.shape
    right = right_ref[...]
    left = left_ref[...]

    def slot_step(slot, carry):
        first = chosen[0, slot]
        second = chosen[1, slot]

        def row_step(step, state):
            ahead, behind, power = state
            base = step * GROUP
            density = window[first, pl.ds(base, GROUP)] * window[second, pl.ds(base, GROUP)]
            value = along_last(density.reshape(GROUP * side, width), right)
            planes = [value[k * side : (k + 1) * side] for k in range(GROUP)]
            planes = along_second(planes, left)
            ratio = decay[0]
            for k in range(GROUP):
                spectrum[slot, base + k] = planes[k]
                ahead = ahead * ratio + planes[k]
                behind = behind + power * planes[k]
                power = power * ratio
            return ahead, behind, power

        zero = jnp.zeros((side, width), jnp.float32)
        ahead, behind, power = lax.fori_loop(
            0, rows // GROUP, row_step, (zero, zero, zero + 1.0)
        )
        moments[slot, 0] = ahead
        moments[slot, 1] = behind
        return carry

    lax.fori_loop(0, chosen[2, 0], slot_step, 0)


def halves(value):
    return pltpu.roll(value, value.shape[-1] // 2, axis=value.ndim - 1)


def packed_moments(moments, power):
    ahead = moments[:, 0]
    behind = moments[:, 1]
    half = ahead.shape[-1] // 2
    ahead_slab = ahead[..., half:] + power[:, half:] * ahead[..., :half]
    behind_slab = behind[..., :half] + power[:, :half] * behind[..., half:]
    return jnp.concatenate([behind_slab, ahead_slab], -1)


def backward_kernel(
    chosen, window, spectrum, moments, mine, other, right_ref, left_ref, decay, out, tail
):
    slots, rows, side, width = spectrum.shape
    right = right_ref[...]
    left = left_ref[...]
    out[...] = jnp.zeros_like(out)
    lower = lax.broadcasted_iota(jnp.int32, (side, width), 1) < width // 2

    def slot_step(slot, carry):
        first = chosen[0, slot]
        second = chosen[1, slot]
        power = decay[1]
        entering = (other[slot] + power * power * mine[slot]) * decay[3]
        ahead_start = halves(entering)
        ahead = jnp.where(lower, ahead_start, halves(moments[slot, 0]) + power * entering)
        behind = jnp.where(lower, halves(moments[slot, 1]) + power * entering, ahead_start)

        def tail_step(step, behind):
            base = rows - (step + 1) * GROUP
            ratio = decay[0]
            for k in reversed(range(GROUP)):
                value = spectrum[slot, base + k]
                spilled = ratio * behind
                tail[base + k] = spilled
                behind = value + spilled
            return behind

        lax.fori_loop(0, rows // GROUP, tail_step, behind)

        def row_step(step, ahead):
            base = step * GROUP
            ratio = decay[0]
            scale = decay[2]
            planes = []
            for k in range(GROUP):
                ahead = spectrum[slot, base + k] + ratio * ahead
                planes.append(scale * (ahead + tail[base + k]))
            planes = along_second(planes, left)
            value = along_last(jnp.concatenate(planes, 0), right)
            potential = value.reshape(GROUP, side, width)
            rows_here = pl.ds(base, GROUP)
            out[first, rows_here] += potential * window[second, rows_here]
            out[second, rows_here] += potential * window[first, rows_here]
            return ahead

        lax.fori_loop(0, rows // GROUP, row_step, ahead)
        return carry

    lax.fori_loop(0, chosen[2, 0], slot_step, 0)


def on_device(orbitals, pair_list, pair_count):
    owned_rows, slab_rows, plane_cells = orbitals.shape
    side = math.isqrt(plane_cells)
    assert lax.axis_size("grid") == 2 and REACH == 2
    rows = slab_rows // 2
    band_count = lax.axis_size("band")
    band_index = lax.axis_index("band")
    even = band_index % 2 == 0
    right, left, decay = tables(side, rows)
    fields = orbitals.reshape(owned_rows, 2, rows, side, side)
    fields = fields.transpose(0, 2, 3, 1, 4).reshape(owned_rows, rows, side, 2 * side)
    far = rotated(fields, "band", -2)
    near = swapped(jnp.where(even, far, fields), "band")
    window = jnp.concatenate([fields, near, far], 0)
    total_rows = window.shape[0]
    pair_rows = pair_list[0]
    slots = pair_rows.shape[0]
    partner = pair_rows[:, 1]
    distance = (partner // owned_rows - band_index) % band_count
    second = jnp.minimum(distance * owned_rows + partner % owned_rows, total_rows - 1)
    chosen = jnp.stack(
        [pair_rows[:, 0], second, jnp.broadcast_to(pair_count[0], second.shape)]
    )
    smem = pl.BlockSpec(memory_space=pltpu.SMEM)
    vmem = pl.BlockSpec(memory_space=pltpu.VMEM)
    params = pltpu.CompilerParams(vmem_limit_bytes=40 * 2**20)
    spectrum, moments = pl.pallas_call(
        forward_kernel,
        out_shape=(
            jax.ShapeDtypeStruct((slots, rows, side, 2 * side), jnp.float32),
            jax.ShapeDtypeStruct((slots, 2, side, 2 * side), jnp.float32),
        ),
        in_specs=[smem, vmem, vmem, vmem, vmem],
        out_specs=(vmem, vmem),
        compiler_params=params,
        name="forward_planes",
    )(chosen, window, right, left, decay)
    mine = packed_moments(moments, decay[1])
    other = swapped(mine, "grid")
    collected = pl.pallas_call(
        backward_kernel,
        out_shape=jax.ShapeDtypeStruct(window.shape, jnp.float32),
        in_specs=[smem, vmem, vmem, vmem, vmem, vmem, vmem, vmem, vmem],
        out_specs=vmem,
        scratch_shapes=[pltpu.VMEM((rows, side, 2 * side), jnp.float32)],
        compiler_params=params,
        name="backward_planes",
    )(chosen, window, spectrum, moments, mine, other, right, left, decay)
    own = collected[:owned_rows]
    passed = swapped(collected[owned_rows : 2 * owned_rows], "band")
    distant = collected[2 * owned_rows :] + jnp.where(even, passed, 0.0)
    own = own + jnp.where(even, 0.0, passed) + rotated(distant, "band", 2)
    own = own.reshape(owned_rows, rows, side, 2, side).transpose(0, 3, 1, 2, 4)
    return own.reshape(orbitals.shape)


def solution(mesh):
    in_specs = (P("band", "grid", None), P("band", None, None), P("band"))
    out_specs = P("band", "grid", None)
    return jax.shard_map(
        on_device, mesh=mesh, in_specs=in_specs, out_specs=out_specs, check_vma=False
    )
```

```python
import functools
import math

import jax
import jax.numpy as jnp
import numpy as np
from jax import lax
from jax.experimental import pallas as pl
from jax.experimental.pallas import tpu as pltpu
from jax.sharding import PartitionSpec as P

REACH = 2
GROUP = 4


def rotated(value, axis, steps):
    count = lax.axis_size(axis)
    pairs = [(source, (source + steps) % count) for source in range(count)]
    return lax.ppermute(value, axis, pairs)


def swapped(value, axis):
    count = lax.axis_size(axis)
    return lax.ppermute(value, axis, [(source, source ^ 1) for source in range(count)])


def split(value):
    high = value.astype(jnp.bfloat16)
    return high, (value - high.astype(jnp.float32)).astype(jnp.bfloat16)


def tables(side, half_rows):
    points = np.arange(side)
    angles = (points[:, None] * points[None, :] % side) * (2.0 * math.pi / side)
    hartley = (np.cos(angles) + np.sin(angles)).astype(np.float32)
    high = hartley.astype(jnp.bfloat16)
    low = (hartley - high.astype(np.float32)).astype(jnp.bfloat16)
    eye = np.eye(2, dtype=np.float32)
    wide_high = np.kron(eye, high.astype(np.float32))
    wide_low = np.kron(eye, low.astype(np.float32))
    right = np.block([[wide_high, wide_low], [wide_high, wide_low]]).astype(jnp.bfloat16)
    left = np.concatenate([high, high, low], 1)
    eigenvalues = 2.0 - 2.0 * np.cos(points * (2.0 * math.pi / side))
    shift = 1.0 / side**2 + eigenvalues[:, None] + np.tile(eigenvalues, 2)[None, :]
    ratio = 1.0 + shift / 2 - np.sqrt(shift + shift**2 / 4)
    power = ratio**half_rows
    reach = ratio**GROUP
    scale = 1.0 / side / (1.0 / ratio - ratio) / side**2
    wrap = 1.0 / (1.0 - power**4)
    decay = np.stack([ratio, power, scale, wrap, reach]).astype(np.float32)
    return right, left, decay


def along_last(value, right):
    width = value.shape[1]
    product = jnp.dot(
        jnp.concatenate(split(value), 1), right, preferred_element_type=jnp.float32
    )
    return product[:, :width] + product[:, width:]


def along_second(planes, left):
    width = planes[0].shape[1]
    out = []
    for start in range(0, len(planes), 2):
        both = jnp.concatenate(planes[start : start + 2], 1)
        high, low = split(both)
        stacked = jnp.concatenate([high, low, high], 0)
        product = jnp.dot(left, stacked, preferred_element_type=jnp.float32)
        out.append(product[:, :width])
        out.append(product[:, width:])
    return out


def halves(value):
    return pltpu.roll(value, value.shape[-1] // 2, axis=value.ndim - 1)


def arrange_kernel(source, *chunks):
    owned, slab_rows, cells = source.shape
    width = chunks[0].shape[-1]
    lower = lax.broadcasted_iota(jnp.int32, (8, width), 1) < width // 2
    parts = 8 // GROUP

    def tile_step(tile, carry):
        lanes = pl.ds(pl.multiple_of(tile * width, width), width)
        for row in range(owned):
            for base in range(0, slab_rows // 2, 8):
                near = source[row, pl.ds(base, 8), lanes]
                far = source[row, pl.ds(base + slab_rows // 2, 8), lanes]
                even = jnp.where(lower, near, halves(far))
                odd = jnp.where(lower, halves(near), far)
                for part in range(parts):
                    chunk = chunks[base // GROUP + part]
                    rows = slice(part * GROUP, (part + 1) * GROUP)
                    chunk[row, :, 2 * tile, :] = even[rows]
                    chunk[row, :, 2 * tile + 1, :] = odd[rows]
        return carry

    lax.fori_loop(0, cells // width, tile_step, 0)


def restore_kernel(flag, *refs):
    out = refs[-1]
    count = (len(refs) - 1) // 3
    own, passed, arrived = refs[:count], refs[count : 2 * count], refs[2 * count : -1]
    owned, slab_rows, cells = out.shape
    width = own[0].shape[-1]
    lower = lax.broadcasted_iota(jnp.int32, (8, width), 1) < width // 2
    parts = 8 // GROUP
    weight = flag[0].astype(jnp.float32)

    def tile_step(tile, carry):
        lanes = pl.ds(pl.multiple_of(tile * width, width), width)
        for row in range(owned):
            for base in range(0, slab_rows // 2, 8):
                lines = []
                for parity in range(2):
                    pieces = []
                    for part in range(parts):
                        c = base // GROUP + part
                        y = 2 * tile + parity
                        pieces.append(
                            own[c][row, :, y, :]
                            + weight * passed[c][row, :, y, :]
                            + arrived[c][row, :, y, :]
                        )
                    lines.append(jnp.concatenate(pieces, 0))
                even, odd = lines
                out[row, pl.ds(base, 8), lanes] = jnp.where(lower, even, halves(odd))
                out[row, pl.ds(base + slab_rows // 2, 8), lanes] = jnp.where(
                    lower, halves(even), odd
                )
        return carry

    lax.fori_loop(0, cells // width, tile_step, 0)


def pick_kernel(flag, after, far, own, out):
    @pl.when(flag[0] == 0)
    def _():
        out[...] = far[...]

    @pl.when(flag[0] == 1)
    def _():
        out[...] = own[...]


def forward_kernel(chosen, after, own, near, far, right_ref, left_ref, decay, spectrum, moments, window):
    slots, rows, side, width = spectrum.shape
    owned = own.shape[0]
    window[:owned] = own[...]
    window[owned : 2 * owned] = near[...]
    window[2 * owned :] = far[...]
    right = right_ref[...]
    left = left_ref[...]

    def slot_step(slot, carry):
        first = chosen[0, slot]
        second = chosen[1, slot]
        density = window[first] * window[second]
        value = along_last(density.reshape(rows * side, width), right)
        planes = [value[k * side : (k + 1) * side] for k in range(rows)]
        planes = along_second(planes, left)
        ratio = decay[0]
        ahead = planes[0]
        behind = planes[-1]
        for k in range(rows):
            spectrum[slot, k] = planes[k]
            if k:
                ahead = ahead * ratio + planes[k]
                behind = behind * ratio + planes[rows - 1 - k]
        moments[slot, 0] = ahead
        moments[slot, 1] = behind
        return carry

    lax.fori_loop(0, chosen[2, 0], slot_step, 0)


def packed_moments(moments, decay):
    power, reach = decay[1], decay[4]
    ahead = moments[0][:, 0]
    behind = moments[-1][:, 1]
    for k in range(1, len(moments)):
        ahead = ahead * reach + moments[k][:, 0]
        behind = behind * reach + moments[-1 - k][:, 1]
    half = ahead.shape[-1] // 2
    ahead_slab = ahead[..., half:] + power[:, half:] * ahead[..., :half]
    behind_slab = behind[..., :half] + power[:, :half] * behind[..., half:]
    return jnp.concatenate([behind_slab, ahead_slab], -1)


def backward_kernel(index, count, chosen, after, older, sent, own, near, far, spectrum, *refs):
    moments = refs[:count]
    mine, other, right_ref, left_ref, decay, kept, handed, distant, window, out = refs[count:]
    slots, rows, side, width = spectrum.shape
    owned = own.shape[0]
    window[:owned] = own[...]
    window[owned : 2 * owned] = near[...]
    window[2 * owned :] = far[...]
    right = right_ref[...]
    left = left_ref[...]
    out[...] = jnp.zeros_like(out)
    lower = lax.broadcasted_iota(jnp.int32, (side, width), 1) < width // 2

    def slot_step(slot, carry):
        first = chosen[0, slot]
        second = chosen[1, slot]
        ratio, power, scale, wrap, reach = [decay[k] for k in range(5)]
        ahead_all = moments[0][slot, 0]
        behind_all = moments[-1][slot, 1]
        for k in range(1, count):
            ahead_all = ahead_all * reach + moments[k][slot, 0]
            behind_all = behind_all * reach + moments[-1 - k][slot, 1]
        entering = (other[slot] + power * power * mine[slot]) * wrap
        turned = halves(entering)
        ahead = jnp.where(lower, turned, halves(ahead_all) + power * entering)
        behind = jnp.where(lower, halves(behind_all) + power * entering, turned)
        for k in range(index):
            ahead = ahead * reach + moments[k][slot, 0]
        for k in reversed(range(index + 1, count)):
            behind = behind * reach + moments[k][slot, 1]
        tails = []
        for k in reversed(range(rows)):
            spilled = ratio * behind
            tails.insert(0, spilled)
            behind = spectrum[slot, k] + spilled
        planes = []
        for k in range(rows):
            ahead = spectrum[slot, k] + ratio * ahead
            planes.append(scale * (ahead + tails[k]))
        planes = along_second(planes, left)
        value = along_last(jnp.concatenate(planes, 0), right)
        potential = value.reshape(rows, side, width)
        out[first] += potential * window[second]
        out[second] += potential * window[first]
        return carry

    lax.fori_loop(0, chosen[2, 0], slot_step, 0)
    kept[...] = out[:owned]
    handed[...] = out[owned : 2 * owned]
    distant[...] = out[2 * owned :]


def on_device(orbitals, pair_list, pair_count):
    owned_rows, slab_rows, plane_cells = orbitals.shape
    side = math.isqrt(plane_cells)
    assert lax.axis_size("grid") == 2 and REACH == 2
    rows = slab_rows // 2
    count = rows // GROUP
    band_count = lax.axis_size("band")
    band_index = lax.axis_index("band")
    even = band_index % 2 == 0
    right, left, decay = tables(side, rows)
    smem = pl.BlockSpec(memory_space=pltpu.SMEM)
    vmem = pl.BlockSpec(memory_space=pltpu.VMEM)
    params = pltpu.CompilerParams(vmem_limit_bytes=12 * 2**20)
    shape = (owned_rows, GROUP, side, 2 * side)
    block = jax.ShapeDtypeStruct(shape, jnp.float32)
    whole = (3 * owned_rows,) + shape[1:]

    def cost(megabytes):
        return pl.CostEstimate(flops=0, bytes_accessed=megabytes << 20, transcendentals=0)

    fields = pl.pallas_call(
        arrange_kernel,
        out_shape=(block,) * count,
        in_specs=[vmem],
        out_specs=(vmem,) * count,
        compiler_params=params,
        cost_estimate=cost(4),
        name="arrange",
    )(orbitals)
    far = [rotated(field, "band", -2) for field in fields]
    flag = (band_index % 2).reshape(1)

    def near_block(index, after):
        picked = pl.pallas_call(
            pick_kernel,
            out_shape=block,
            in_specs=[smem, vmem, vmem, vmem],
            out_specs=vmem,
            compiler_params=params,
            cost_estimate=cost(1),
            name="pick",
        )(flag, after, far[index], fields[index])
        return swapped(picked, "band")

    near = [near_block(c, fields[c]) for c in range(2)]
    pair_rows = pair_list[0]
    slots = pair_rows.shape[0]
    partner = pair_rows[:, 1]
    distance = (partner // owned_rows - band_index) % band_count
    second = jnp.minimum(distance * owned_rows + partner % owned_rows, 3 * owned_rows - 1)
    chosen = jnp.stack(
        [pair_rows[:, 0], second, jnp.broadcast_to(pair_count[0], second.shape)]
    )
    spectra, moments = [], []
    for c in range(count):
        spectrum, moment = pl.pallas_call(
            forward_kernel,
            out_shape=(
                jax.ShapeDtypeStruct((slots,) + shape[1:], jnp.float32),
                jax.ShapeDtypeStruct((slots, 2, side, 2 * side), jnp.float32),
            ),
            in_specs=[smem] + [vmem] * 7,
            out_specs=(vmem, vmem),
            scratch_shapes=[pltpu.VMEM(whole, jnp.float32)],
            compiler_params=params,
            cost_estimate=cost(1),
            name="forward_planes",
        )(chosen, moments[-1] if c else fields[c], fields[c], near[c], far[c], right, left, decay)
        spectra.append(spectrum)
        moments.append(moment)
        if c + 2 < count:
            near.append(near_block(c + 2, moment))
    mine = packed_moments(moments, decay)
    other = swapped(mine, "grid")
    own, passed, joined, arrived = [], [], [], []
    for c in range(count):
        kept, handed, distant = pl.pallas_call(
            functools.partial(backward_kernel, c, count),
            out_shape=(block,) * 3,
            in_specs=[smem] + [vmem] * (12 + count),
            out_specs=(vmem,) * 3,
            scratch_shapes=[pltpu.VMEM(whole, jnp.float32)] * 2,
            compiler_params=params,
            cost_estimate=cost(1),
            name="backward_planes",
        )(
            chosen, own[-1] if c else mine, joined[c - 2] if c > 1 else mine,
            arrived[c - 3] if c > 2 else mine,
            fields[c], near[c], far[c], spectra[c], *moments,
            mine, other, right, left, decay,
        )
        handed = swapped(handed, "band")
        own.append(kept)
        passed.append(handed)
        joined.append(distant + jnp.where(even, handed, 0.0))
        arrived.append(rotated(joined[-1], "band", 2))
    return pl.pallas_call(
        restore_kernel,
        out_shape=jax.ShapeDtypeStruct(orbitals.shape, jnp.float32),
        in_specs=[smem] + [vmem] * (3 * count),
        out_specs=vmem,
        compiler_params=params,
        cost_estimate=cost(6),
        name="restore",
    )(flag, *own, *passed, *arrived)


def solution(mesh):
    in_specs = (P("band", "grid", None), P("band", None, None), P("band"))
    out_specs = P("band", "grid", None)
    return jax.shard_map(
        on_device, mesh=mesh, in_specs=in_specs, out_specs=out_specs, check_vma=False
    )
```

```python
import functools
import math

import jax
import jax.numpy as jnp
import numpy as np
from jax import lax
from jax.experimental import pallas as pl
from jax.experimental.pallas import tpu as pltpu
from jax.sharding import PartitionSpec as P

REACH = 2
GROUP = 8


def rotated(value, axis, steps):
    count = lax.axis_size(axis)
    pairs = [(source, (source + steps) % count) for source in range(count)]
    return lax.ppermute(value, axis, pairs)


def swapped(value, axis):
    count = lax.axis_size(axis)
    return lax.ppermute(value, axis, [(source, source ^ 1) for source in range(count)])


def split(value):
    high = value.astype(jnp.bfloat16)
    return high, (value - high.astype(jnp.float32)).astype(jnp.bfloat16)


def tables(side, half_rows):
    points = np.arange(side)
    angles = (points[:, None] * points[None, :] % side) * (2.0 * math.pi / side)
    hartley = (np.cos(angles) + np.sin(angles)).astype(np.float32)
    high = hartley.astype(jnp.bfloat16)
    low = (hartley - high.astype(np.float32)).astype(jnp.bfloat16)
    eye = np.eye(2, dtype=np.float32)
    wide_high = np.kron(eye, high.astype(np.float32))
    wide_low = np.kron(eye, low.astype(np.float32))
    right = np.block([[wide_high, wide_low], [wide_high, wide_low]]).astype(jnp.bfloat16)
    left = np.concatenate([high, high, low], 1)
    eigenvalues = 2.0 - 2.0 * np.cos(points * (2.0 * math.pi / side))
    shift = 1.0 / side**2 + eigenvalues[:, None] + np.tile(eigenvalues, 2)[None, :]
    ratio = 1.0 + shift / 2 - np.sqrt(shift + shift**2 / 4)
    power = ratio**half_rows
    reach = ratio**GROUP
    scale = 1.0 / side / (1.0 / ratio - ratio) / side**2
    wrap = 1.0 / (1.0 - power**4)
    decay = np.stack([ratio, power, scale, wrap, reach]).astype(np.float32)
    return right, left, decay


def along_last(value, right):
    width = value.shape[1]
    product = jnp.dot(
        jnp.concatenate(split(value), 1), right, preferred_element_type=jnp.float32
    )
    return product[:, :width] + product[:, width:]


def along_second(planes, left):
    width = planes[0].shape[1]
    out = []
    for start in range(0, len(planes), 2):
        both = jnp.concatenate(planes[start : start + 2], 1)
        high, low = split(both)
        stacked = jnp.concatenate([high, low, high], 0)
        product = jnp.dot(left, stacked, preferred_element_type=jnp.float32)
        out.append(product[:, :width])
        out.append(product[:, width:])
    return out


def halves(value):
    return pltpu.roll(value, value.shape[-1] // 2, axis=value.ndim - 1)


def arrange_kernel(index, after, source, chunk):
    owned, slab_rows, cells = source.shape
    width = chunk.shape[-1]
    lower = lax.broadcasted_iota(jnp.int32, (GROUP, width), 1) < width // 2
    tiles = 4

    def tile_step(step, carry):
        for row in range(owned):
            lines = []
            for k in range(tiles):
                lanes = pl.ds(pl.multiple_of((step * tiles + k) * width, width), width)
                near = source[row, pl.ds(index * GROUP, GROUP), lanes]
                far = source[row, pl.ds(index * GROUP + slab_rows // 2, GROUP), lanes]
                lines.append(jnp.where(lower, near, halves(far)))
                lines.append(jnp.where(lower, halves(near), far))
            block = jnp.swapaxes(jnp.stack(lines, 0), 0, 1)
            chunk[row, :, pl.ds(pl.multiple_of(step * 2 * tiles, 2 * tiles), 2 * tiles), :] = block
        return carry

    lax.fori_loop(0, cells // (width * tiles), tile_step, 0)


def restore_kernel(flag, *refs):
    out = refs[-1]
    count = (len(refs) - 1) // 3
    own, passed, arrived = refs[:count], refs[count : 2 * count], refs[2 * count : -1]
    owned, slab_rows, cells = out.shape
    width = own[0].shape[-1]
    lower = lax.broadcasted_iota(jnp.int32, (GROUP, width), 1) < width // 2
    weight = flag[0].astype(jnp.float32)
    tiles = 4

    def tile_step(step, carry):
        ys = pl.ds(pl.multiple_of(step * 2 * tiles, 2 * tiles), 2 * tiles)
        for row in range(owned):
            for c in range(count):
                block = (
                    own[c][row, :, ys, :]
                    + weight * passed[c][row, :, ys, :]
                    + arrived[c][row, :, ys, :]
                )
                block = jnp.swapaxes(block, 0, 1)
                for k in range(tiles):
                    lanes = pl.ds(pl.multiple_of((step * tiles + k) * width, width), width)
                    even, odd = block[2 * k], block[2 * k + 1]
                    out[row, pl.ds(c * GROUP, GROUP), lanes] = jnp.where(
                        lower, even, halves(odd)
                    )
                    out[row, pl.ds(c * GROUP + slab_rows // 2, GROUP), lanes] = jnp.where(
                        lower, halves(even), odd
                    )
        return carry

    lax.fori_loop(0, cells // (width * tiles), tile_step, 0)


def pick_kernel(flag, after, far, own, out):
    @pl.when(flag[0] == 0)
    def _():
        out[...] = far[...]

    @pl.when(flag[0] == 1)
    def _():
        out[...] = own[...]


def join_kernel(flag, after, distant, handed, out):
    weight = 1.0 - flag[0].astype(jnp.float32)
    out[...] = distant[...] + weight * handed[...]


def forward_kernel(chosen, after, own, near, far, right_ref, left_ref, decay, spectrum, moments, window):
    slots, rows, side, width = spectrum.shape
    owned = own.shape[0]
    window[:owned] = own[...]
    window[owned : 2 * owned] = near[...]
    window[2 * owned :] = far[...]
    right = right_ref[...]
    left = left_ref[...]

    def slot_step(slot, carry):
        first = chosen[0, slot]
        second = chosen[1, slot]
        density = window[first] * window[second]
        value = along_last(density.reshape(rows * side, width), right)
        planes = [value[k * side : (k + 1) * side] for k in range(rows)]
        planes = along_second(planes, left)
        ratio = decay[0]
        ahead = planes[0]
        behind = planes[-1]
        for k in range(rows):
            spectrum[slot, k] = planes[k]
            if k:
                ahead = ahead * ratio + planes[k]
                behind = behind * ratio + planes[rows - 1 - k]
        moments[slot, 0] = ahead
        moments[slot, 1] = behind
        return carry

    lax.fori_loop(0, chosen[2, 0], slot_step, 0)


def packed_moments(moments, decay):
    power, reach = decay[1], decay[4]
    ahead = moments[0][:, 0]
    behind = moments[-1][:, 1]
    for k in range(1, len(moments)):
        ahead = ahead * reach + moments[k][:, 0]
        behind = behind * reach + moments[-1 - k][:, 1]
    half = ahead.shape[-1] // 2
    ahead_slab = ahead[..., half:] + power[:, half:] * ahead[..., :half]
    behind_slab = behind[..., :half] + power[:, :half] * behind[..., half:]
    return jnp.concatenate([behind_slab, ahead_slab], -1)


def backward_kernel(index, count, chosen, after, older, sent, own, near, far, spectrum, *refs):
    moments = refs[:count]
    mine, other, right_ref, left_ref, decay, kept, handed, distant, window, out = refs[count:]
    slots, rows, side, width = spectrum.shape
    owned = own.shape[0]
    window[:owned] = own[...]
    window[owned : 2 * owned] = near[...]
    window[2 * owned :] = far[...]
    right = right_ref[...]
    left = left_ref[...]
    out[...] = jnp.zeros_like(out)
    lower = lax.broadcasted_iota(jnp.int32, (side, width), 1) < width // 2

    def slot_step(slot, carry):
        first = chosen[0, slot]
        second = chosen[1, slot]
        ratio, power, scale, wrap, reach = [decay[k] for k in range(5)]
        ahead_all = moments[0][slot, 0]
        behind_all = moments[-1][slot, 1]
        for k in range(1, count):
            ahead_all = ahead_all * reach + moments[k][slot, 0]
            behind_all = behind_all * reach + moments[-1 - k][slot, 1]
        entering = (other[slot] + power * power * mine[slot]) * wrap
        turned = halves(entering)
        ahead = jnp.where(lower, turned, halves(ahead_all) + power * entering)
        behind = jnp.where(lower, halves(behind_all) + power * entering, turned)
        for k in range(index):
            ahead = ahead * reach + moments[k][slot, 0]
        for k in reversed(range(index + 1, count)):
            behind = behind * reach + moments[k][slot, 1]
        tails = []
        for k in reversed(range(rows)):
            spilled = ratio * behind
            tails.insert(0, spilled)
            behind = spectrum[slot, k] + spilled
        planes = []
        for k in range(rows):
            ahead = spectrum[slot, k] + ratio * ahead
            planes.append(scale * (ahead + tails[k]))
        planes = along_second(planes, left)
        value = along_last(jnp.concatenate(planes, 0), right)
        potential = value.reshape(rows, side, width)
        out[first] += potential * window[second]
        out[second] += potential * window[first]
        return carry

    lax.fori_loop(0, chosen[2, 0], slot_step, 0)
    kept[...] = out[:owned]
    handed[...] = out[owned : 2 * owned]
    distant[...] = out[2 * owned :]


def on_device(orbitals, pair_list, pair_count):
    owned_rows, slab_rows, plane_cells = orbitals.shape
    side = math.isqrt(plane_cells)
    assert lax.axis_size("grid") == 2 and REACH == 2
    rows = slab_rows // 2
    count = rows // GROUP
    band_count = lax.axis_size("band")
    band_index = lax.axis_index("band")
    even = band_index % 2 == 0
    right, left, decay = tables(side, rows)
    smem = pl.BlockSpec(memory_space=pltpu.SMEM)
    vmem = pl.BlockSpec(memory_space=pltpu.VMEM)
    params = pltpu.CompilerParams(vmem_limit_bytes=12 * 2**20)
    shape = (owned_rows, GROUP, side, 2 * side)
    block = jax.ShapeDtypeStruct(shape, jnp.float32)
    whole = (3 * owned_rows,) + shape[1:]

    def cost(megabytes):
        return pl.CostEstimate(flops=0, bytes_accessed=megabytes << 20, transcendentals=0)

    fields, after = [], orbitals
    for c in range(count):
        after = pl.pallas_call(
            functools.partial(arrange_kernel, c),
            out_shape=block,
            in_specs=[vmem, vmem],
            out_specs=vmem,
            compiler_params=params,
            cost_estimate=cost(1),
            name="arrange",
        )(after, orbitals)
        fields.append(after)
    far = [rotated(field, "band", -2) for field in fields]
    flag = (band_index % 2).reshape(1)

    def near_block(index, after):
        picked = pl.pallas_call(
            pick_kernel,
            out_shape=block,
            in_specs=[smem, vmem, vmem, vmem],
            out_specs=vmem,
            compiler_params=params,
            cost_estimate=cost(1),
            name="pick",
        )(flag, after, far[index], fields[index])
        return swapped(picked, "band")

    near = [near_block(0, fields[0])]
    pair_rows = pair_list[0]
    slots = pair_rows.shape[0]
    partner = pair_rows[:, 1]
    distance = (partner // owned_rows - band_index) % band_count
    second = jnp.minimum(distance * owned_rows + partner % owned_rows, 3 * owned_rows - 1)
    chosen = jnp.stack(
        [pair_rows[:, 0], second, jnp.broadcast_to(pair_count[0], second.shape)]
    )
    spectra, moments = [], []
    for c in range(count):
        spectrum, moment = pl.pallas_call(
            forward_kernel,
            out_shape=(
                jax.ShapeDtypeStruct((slots,) + shape[1:], jnp.float32),
                jax.ShapeDtypeStruct((slots, 2, side, 2 * side), jnp.float32),
            ),
            in_specs=[smem] + [vmem] * 7,
            out_specs=(vmem, vmem),
            scratch_shapes=[pltpu.VMEM(whole, jnp.float32)],
            compiler_params=params,
            cost_estimate=cost(1),
            name="forward_planes",
        )(chosen, moments[-1] if c else fields[c], fields[c], near[c], far[c], right, left, decay)
        spectra.append(spectrum)
        moments.append(moment)
        if c + 1 < count:
            near.append(near_block(c + 1, moment))
    mine = packed_moments(moments, decay)
    other = swapped(mine, "grid")
    own, passed, joined, arrived = [], [], [], []
    for c in range(count):
        kept, handed, distant = pl.pallas_call(
            functools.partial(backward_kernel, c, count),
            out_shape=(block,) * 3,
            in_specs=[smem] + [vmem] * (12 + count),
            out_specs=(vmem,) * 3,
            scratch_shapes=[pltpu.VMEM(whole, jnp.float32)] * 2,
            compiler_params=params,
            cost_estimate=cost(1),
            name="backward_planes",
        )(
            chosen, own[-1] if c else mine, joined[c - 2] if c > 1 else mine,
            arrived[c - 3] if c > 2 else mine,
            fields[c], near[c], far[c], spectra[c], *moments,
            mine, other, right, left, decay,
        )
        handed = swapped(handed, "band")
        own.append(kept)
        passed.append(handed)
        total = pl.pallas_call(
            join_kernel,
            out_shape=block,
            in_specs=[smem] + [vmem] * 3,
            out_specs=vmem,
            compiler_params=params,
            cost_estimate=cost(1),
            name="join",
        )(flag, arrived[-1] if c else kept, distant, handed)
        joined.append(total)
        arrived.append(rotated(joined[-1], "band", 2))
    return pl.pallas_call(
        restore_kernel,
        out_shape=jax.ShapeDtypeStruct(orbitals.shape, jnp.float32),
        in_specs=[smem] + [vmem] * (3 * count),
        out_specs=vmem,
        compiler_params=params,
        cost_estimate=cost(6),
        name="restore",
    )(flag, *own, *passed, *arrived)


def solution(mesh):
    in_specs = (P("band", "grid", None), P("band", None, None), P("band"))
    out_specs = P("band", "grid", None)
    return jax.shard_map(
        on_device, mesh=mesh, in_specs=in_specs, out_specs=out_specs, check_vma=False
    )
```
